32 devices in a mesh: dp: 8 (over z, core), row: 2 (over x), col: 2 (over y).
Axes of the slice: x: 2, y: 2, z: 4, core: 2. Of those that a mesh axis runs over, the one named last changes fastest.
Arguments:
- tokens: bfloat16 [4096, 8192], P(('dp', 'row', 'col')), parts along dimension 0, may hold values from -6 to 6
- w_gate: bfloat16 [8192, 1024], P(('row', 'col')), may hold values from -0.0625 to 0.0625
- w_up: bfloat16 [8192, 1024], P(('row', 'col')), may hold values from -0.0625 to 0.0625
- w_down: bfloat16 [1024, 8192], P(None, ('row', 'col')), may hold values from -0.1875 to 0.1875
Outputs:
- mixed: bfloat16 [4096, 8192], P(('dp', 'row', 'col')), parts along dimension 0
The draws below stay inside these ranges and needn't reach their ends.
There are 8 independent parts, one for each index of `dp`. The reference program is written for one: setup_inputs(seed, part) draws one part's arguments, and reference() takes and returns one part's arrays. A program takes and returns all parts, laid end to end along the dimension named above; an argument that names none is the same for every part. Nothing has to cross between parts.
All inputs are finite; a program needn't handle non-finite values.
Results may differ from the reference program's by a relative error of at most 0.029.
Values may be sent and summed in bfloat16 or wider, within the bound.
A program may use at most 64 MiB of HBM per device.

```python
import jax
import jax.numpy as jnp
from jax import lax

D = 8192
H = 1024
TOKENS = 512
N_ROW = 2


def block_scale(rng, shape, pieces, low, largest):
    loudness = 1.0
    for axis_at, shards_of in pieces:
        draws = jax.random.uniform(jax.random.fold_in(jax.random.fold_in(rng, 6), axis_at), (shards_of,), jnp.float32, low / len(pieces), largest / len(pieces))
        loudness = loudness * jnp.repeat(jnp.exp(draws), shape[axis_at] // shards_of).reshape((-1,) + (1,) * (len(shape) - 1 - axis_at))
    return loudness


def noise(own_key, shape, width, bound, shards=(), dtype=jnp.bfloat16):
    level = block_scale(own_key, shape, shards, -0.22, 0.18) if shards else 1.0
    entries = jax.random.normal(own_key, shape, jnp.float32) * width * level
    return jnp.minimum(jnp.maximum(entries, -bound), bound).astype(dtype)


def setup_inputs(seed: int = 0, part: int = 0) -> dict:
    seeds = jax.random.split(jax.random.key(seed), 5)
    part_splits = jax.random.split(jax.random.fold_in(seeds[4], part), 5)
    return {
        "tokens": noise(part_splits[0], (TOKENS, D), 1.0, 6.0, ((0, 4),)),
        "w_gate": noise(seeds[1], (D, H), D ** -0.5, 0.0625, ((0, 4),)),
        "w_up": noise(seeds[2], (D, H), D ** -0.5, 0.0625, ((0, 4),)),
        "w_down": noise(seeds[3], (H, D), H ** -0.5, 0.1875, ((1, 4),)),
    }


def reference(tokens, w_gate, w_up, w_down):
    slab_width = D // N_ROW
    paired = jnp.concatenate([w_gate, w_up], axis=1)
    running = jnp.zeros((tokens.shape[0], 2 * H), jnp.float32)
    for block_index in range(N_ROW):
        lower = block_index * slab_width
        upper = lower + slab_width
        partial_value = jnp.dot(tokens[:, lower:upper], paired[lower:upper], preferred_element_type=jnp.float32)
        rounded = lax.optimization_barrier(partial_value.astype(jnp.bfloat16))
        running = running + rounded.astype(jnp.float32)
    hidden = (jax.nn.silu(running[:, :H]) * running[:, H:]).astype(jnp.bfloat16)
    return jnp.dot(hidden, w_down, preferred_element_type=jnp.float32).astype(jnp.bfloat16)
```

```python
import functools

import jax
import jax.numpy as jnp
from jax import lax
from jax.experimental import pallas as pl
from jax.experimental.pallas import tpu as pltpu
from jax.sharding import PartitionSpec as P

MESH = pl.DeviceIdType.MESH
CHUNKS = 2


def tile_of(width, most):
    tile = min(width, most)
    while width % tile:
        tile //= 2
    return tile


def kernel(
    rows, cols, chunks,
    x_ref, wg_ref, wu_ref, wd_ref, out_ref,
    wg, wu, wd, xbuf, acc, psend, prec, hbuf, osend,
    w_sem, x_send, x_recv, p_send, p_recv, h_send, h_recv, o_send, o_recv,
):
    n = rows * cols
    row, col = lax.axis_index("row"), lax.axis_index("col")
    me = row * cols + col
    tokens = x_ref.shape[0]
    t = tokens // chunks
    features = wg.shape[0]
    hidden = wg.shape[1]
    out_cols = wd.shape[1]
    bf16, f32 = jnp.bfloat16, jnp.float32

    def worker(o):
        r = lax.rem(row + o // cols, rows)
        c = lax.rem(col + lax.rem(o, cols), cols)
        return r, c

    def owner(o):
        r = lax.rem(row - o // cols + rows, rows)
        c = lax.rem(col - lax.rem(o, cols) + cols, cols)
        return r, c

    def at(rc):
        return {"row": rc[0], "col": rc[1]}

    def x_copy(c, o):
        r_, c_ = worker(o)
        start = pl.multiple_of((r_ * cols + c_) * features, features)
        return pltpu.make_async_remote_copy(
            src_ref=x_ref.at[pl.ds(c * t, t), pl.ds(start, features)],
            dst_ref=xbuf.at[c, o],
            send_sem=x_send.at[c, o], recv_sem=x_recv.at[c, o],
            device_id=at((r_, c_)), device_id_type=MESH,
        )

    def x_own(c):
        start = pl.multiple_of(me * features, features)
        return pltpu.make_async_copy(
            x_ref.at[pl.ds(c * t, t), pl.ds(start, features)], xbuf.at[c, 0], x_recv.at[c, 0]
        )

    def p_copy(c, o):
        return pltpu.make_async_remote_copy(
            src_ref=psend.at[c, o], dst_ref=prec.at[c, o],
            send_sem=p_send.at[c, o], recv_sem=p_recv.at[c, o],
            device_id=at(owner(o)), device_id_type=MESH,
        )

    def h_copy(c, o):
        return pltpu.make_async_remote_copy(
            src_ref=hbuf.at[c, 0], dst_ref=hbuf.at[c, o],
            send_sem=h_send.at[c, o], recv_sem=h_recv.at[c, o],
            device_id=at(worker(o)), device_id_type=MESH,
        )

    def o_copy(c, o):
        start = pl.multiple_of(me * out_cols, out_cols)
        return pltpu.make_async_remote_copy(
            src_ref=osend.at[c, o],
            dst_ref=out_ref.at[pl.ds(c * t, t), pl.ds(start, out_cols)],
            send_sem=o_send.at[c, o], recv_sem=o_recv.at[c, o],
            device_id=at(owner(o)), device_id_type=MESH,
        )

    def o_arrival(c, o):
        r_, c_ = worker(o)
        start = pl.multiple_of((r_ * cols + c_) * out_cols, out_cols)
        return pltpu.make_async_remote_copy(
            src_ref=osend.at[c, o],
            dst_ref=out_ref.at[pl.ds(c * t, t), pl.ds(start, out_cols)],
            send_sem=o_send.at[c, o], recv_sem=o_recv.at[c, o],
            device_id=at(owner(o)), device_id_type=MESH,
        )

    def o_own(c):
        start = pl.multiple_of(me * out_cols, out_cols)
        return pltpu.make_async_copy(
            osend.at[c, 0], out_ref.at[pl.ds(c * t, t), pl.ds(start, out_cols)], o_recv.at[c, 0]
        )

    loads = [
        pltpu.make_async_copy(wg_ref, wg, w_sem.at[0]),
        pltpu.make_async_copy(wu_ref, wu, w_sem.at[1]),
        pltpu.make_async_copy(wd_ref, wd, w_sem.at[2]),
    ]

    barrier = pltpu.get_barrier_semaphore()
    for o in range(1, n):
        pl.semaphore_signal(barrier, inc=1, device_id=at(worker(o)), device_id_type=MESH)
    pl.semaphore_wait(barrier, n - 1)

    for c in range(chunks):
        for o in range(1, n):
            x_copy(c, o).start()
    for c in range(chunks):
        x_own(c).start()
    for load in loads:
        load.start()
    loads[0].wait()
    loads[1].wait()

    up_tile = tile_of(hidden, 512)

    def first(i, _):
        c, o = i // n, lax.rem(i, n)

        @pl.when(o == 0)
        def _():
            x_own(c).wait()

        @pl.when(o != 0)
        def _():
            x_copy(c, o).wait_recv()

        def tile(j, _):
            at_gate = pl.multiple_of(j * up_tile, up_tile)
            at_up = pl.multiple_of(hidden + j * up_tile, up_tile)
            gate = jnp.dot(xbuf[c, o], wg[:, pl.ds(at_gate, up_tile)], preferred_element_type=f32)
            up = jnp.dot(xbuf[c, o], wu[:, pl.ds(at_gate, up_tile)], preferred_element_type=f32)

            @pl.when(o == 0)
            def _():
                acc[c, :, pl.ds(at_gate, up_tile)] = gate
                acc[c, :, pl.ds(at_up, up_tile)] = up

            @pl.when(o != 0)
            def _():
                psend[c, o, :, pl.ds(at_gate, up_tile)] = gate.astype(bf16)
                psend[c, o, :, pl.ds(at_up, up_tile)] = up.astype(bf16)

            return 0

        lax.fori_loop(0, hidden // up_tile, tile, 0)

        @pl.when(o != 0)
        def _():
            p_copy(c, o).start()

        return 0

    lax.fori_loop(0, n * chunks, first, 0)

    sub = tile_of(t, 16)

    def second(c, _):
        def arrive(o, _):
            p_copy(c, o).wait_recv()
            return 0

        lax.fori_loop(1, n, arrive, 0)

        def block(b, _):
            at_row = pl.ds(pl.multiple_of(b * sub, sub), sub)
            gate = acc[c, at_row, pl.ds(0, hidden)]
            up = acc[c, at_row, pl.ds(hidden, hidden)]
            for o in range(1, n):
                gate = gate + prec[c, o, at_row, pl.ds(0, hidden)].astype(f32)
                up = up + prec[c, o, at_row, pl.ds(hidden, hidden)].astype(f32)
            hbuf[c, 0, at_row, :] = (gate / (1.0 + jnp.exp(-gate)) * up).astype(bf16)
            return 0

        lax.fori_loop(0, t // sub, block, 0)
        for o in range(1, n):
            h_copy(c, o).start()
        return 0

    lax.fori_loop(0, chunks, second, 0)

    loads[2].wait()
    down_tile = tile_of(out_cols, 512)

    def third(i, _):
        c, o = i // n, lax.rem(i, n)

        @pl.when(o != 0)
        def _():
            h_copy(c, o).wait_recv()

        def tile(j, _):
            where = pl.ds(pl.multiple_of(j * down_tile, down_tile), down_tile)
            osend[c, o, :, where] = jnp.dot(
                hbuf[c, o], wd[:, where], preferred_element_type=f32
            ).astype(bf16)
            return 0

        lax.fori_loop(0, out_cols // down_tile, tile, 0)

        @pl.when(o == 0)
        def _():
            o_own(c).start()

        @pl.when(o != 0)
        def _():
            o_copy(c, o).start()

        return 0

    lax.fori_loop(0, n * chunks, third, 0)

    for c in range(chunks):
        o_own(c).wait()
        for o in range(1, n):
            x_copy(c, o).wait_send()
            p_copy(c, o).wait_send()
            h_copy(c, o).wait_send()
            o_copy(c, o).wait_send()
            o_arrival(c, o).wait_recv()


def solution(mesh):
    rows, cols = mesh.shape["row"], mesh.shape["col"]
    n = rows * cols

    def shards(tokens, w_gate, w_up, w_down):
        count, width = tokens.shape
        features, hidden = w_gate.shape
        out_cols = w_down.shape[1]
        chunks = CHUNKS
        t = count // chunks
        bf16 = jnp.bfloat16
        pair = pltpu.SemaphoreType.DMA((chunks, n))
        any_space = pl.BlockSpec(memory_space=pl.ANY)
        return pl.pallas_call(
            functools.partial(kernel, rows, cols, chunks),
            out_shape=jax.ShapeDtypeStruct((count, width), bf16),
            in_specs=[any_space] * 4,
            out_specs=any_space,
            scratch_shapes=[
                pltpu.VMEM((features, hidden), bf16),
                pltpu.VMEM((features, hidden), bf16),
                pltpu.VMEM((hidden, out_cols), bf16),
                pltpu.VMEM((chunks, n, t, features), bf16),
                pltpu.VMEM((chunks, t, 2 * hidden), jnp.float32),
                pltpu.VMEM((chunks, n, t, 2 * hidden), bf16),
                pltpu.VMEM((chunks, n, t, 2 * hidden), bf16),
                pltpu.VMEM((chunks, n, t, hidden), bf16),
                pltpu.VMEM((chunks, n, t, out_cols), bf16),
                pltpu.SemaphoreType.DMA((3,)),
                pair, pair, pair, pair, pair, pair, pair, pair,
            ],
            compiler_params=pltpu.CompilerParams(collective_id=0, has_side_effects=True),
        )(tokens, w_gate, w_up, w_down)

    in_specs = (
        P(("dp", "row", "col"), None),
        P(("row", "col"), None),
        P(("row", "col"), None),
        P(None, ("row", "col")),
    )
    out_specs = P(("dp", "row", "col"), None)
    return jax.shard_map(shards, mesh=mesh, in_specs=in_specs, out_specs=out_specs, check_vma=False)
```

```python
import functools

import jax
import jax.numpy as jnp
from jax import lax
from jax.experimental import pallas as pl
from jax.experimental.pallas import tpu as pltpu
from jax.sharding import PartitionSpec as P

MESH = pl.DeviceIdType.MESH
CHUNKS = 4
AHEAD = 2


def tile_of(width, most):
    tile = min(width, most)
    while width % tile:
        tile //= 2
    return tile


def kernel(
    rows, cols, chunks,
    x_ref, wg_ref, wu_ref, wd_ref, out_ref,
    wg, wu, wd, xbuf, acc, part, rec_a, rec_b, sum_a, sum_b, fin_a, fin_b, hbuf, osend,
    w_sem, x_sem, a_sem, b_sem, c_sem, d_sem, h_sem, ra_sem, rb_sem, o_sem,
):
    n = rows * cols
    row, col = lax.axis_index("row"), lax.axis_index("col")
    me = row * cols + col
    t = x_ref.shape[0] // chunks
    features, hidden = wg.shape
    half = hidden // 2
    out_cols = wd.shape[1]
    bf16, f32 = jnp.bfloat16, jnp.float32

    def up(r, c):
        return lax.rem(row + r, rows), lax.rem(col + c, cols)

    def down(r, c):
        return lax.rem(row + rows - r, rows), lax.rem(col + cols - c, cols)

    def shard(rc, width):
        return pl.ds(pl.multiple_of((rc[0] * cols + rc[1]) * width, width), width)

    def remote(src, dst, sems, index, to):
        return pltpu.make_async_remote_copy(
            src_ref=src, dst_ref=dst,
            send_sem=sems.at[(0, *index)], recv_sem=sems.at[(1, *index)],
            device_id={"row": to[0], "col": to[1]}, device_id_type=MESH,
        )

    def tok(k):
        return pl.ds(pl.multiple_of(k * t, t), t)

    slots = [(r, c) for r in range(rows) for c in range(cols)]
    others = slots[1:]

    def at_slot(r, c):
        return pl.ds((r * cols + c) * t, t)

    def x_copy(k, r, c):
        to = up(r, c)
        return remote(
            x_ref.at[tok(k), shard(to, features)], xbuf.at[k, at_slot(r, c)],
            x_sem, (k, r * cols + c), to,
        )

    def x_own(k):
        return pltpu.make_async_copy(
            x_ref.at[tok(k), shard((row, col), features)], xbuf.at[k, at_slot(0, 0)], x_sem.at[1, k, 0]
        )

    def a_copy(k, r):
        return remote(part.at[k, 0, r], rec_a.at[k, r], a_sem, (k, r), down(r, 0))

    def b_copy(k, c):
        return remote(part.at[k, 1, :, c], rec_b.at[k, c], b_sem, (k, c), down(0, c))

    def c_copy(k, c):
        return remote(sum_a.at[k, c], fin_a.at[k, c], c_sem, (k, c), down(0, c))

    def d_copy(k, r):
        return remote(sum_b.at[k, r], fin_b.at[k, r], d_sem, (k, r), down(r, 0))

    def h_copy(k, r, c):
        return remote(
            hbuf.at[k, at_slot(0, 0)], hbuf.at[k, at_slot(r, c)], h_sem, (k, r * cols + c), up(r, c)
        )

    def relay_a(k, r, c):
        return remote(
            hbuf.at[k, at_slot(r, 0), pl.ds(0, half)], hbuf.at[k, at_slot(r, c), pl.ds(0, half)],
            ra_sem, (k, r * cols + c), up(0, c),
        )

    def relay_b(k, r, c):
        return remote(
            hbuf.at[k, at_slot(0, c), pl.ds(half, half)], hbuf.at[k, at_slot(r, c), pl.ds(half, half)],
            rb_sem, (k, r * cols + c), up(r, 0),
        )

    def o_copy(k, r, c, columns_of):
        return remote(
            osend.at[k, at_slot(r, c)], out_ref.at[tok(k), shard(columns_of, out_cols)],
            o_sem, (k, r * cols + c), down(r, c),
        )

    def o_own(k):
        return pltpu.make_async_copy(
            osend.at[k, at_slot(0, 0)], out_ref.at[tok(k), shard((row, col), out_cols)], o_sem.at[1, k, 0]
        )

    edges = [(r, c) for r, c in others if r == 0 or c == 0]
    corners = [(r, c) for r, c in others if r and c]

    loads = [
        pltpu.make_async_copy(wg_ref, wg, w_sem.at[0]),
        pltpu.make_async_copy(wu_ref, wu, w_sem.at[1]),
        pltpu.make_async_copy(wd_ref, wd, w_sem.at[2]),
    ]

    barrier = pltpu.get_barrier_semaphore()
    for r, c in others:
        to = up(r, c)
        pl.semaphore_signal(barrier, inc=1, device_id={"row": to[0], "col": to[1]}, device_id_type=MESH)
    pl.semaphore_wait(barrier, n - 1)

    def send_tokens(k):
        for r, c in others:
            x_copy(k, r, c).start()

    for k in range(min(AHEAD, chunks)):
        send_tokens(k)
    for k in range(chunks):
        x_own(k).start()
    for load in loads:
        load.start()
    loads[0].wait()
    loads[1].wait()

    tile = tile_of(half, 512)
    per_half = half // tile

    def project(k):
        x_own(k).wait()
        for r, c in others:
            x_copy(k, r, c).wait_recv()

        def column(j, _):
            side, at = j // per_half, lax.rem(j, per_half) * tile
            source = pl.ds(pl.multiple_of(j * tile, tile), tile)
            for w, base in ((wg, 0), (wu, half)):
                target = pl.ds(pl.multiple_of(base + at, tile), tile)
                got = jnp.dot(xbuf[k], w[:, source], preferred_element_type=f32)
                acc[k, side, :, target] = got[:t]
                for r, c in others:
                    first = (r * cols + c) * t
                    part[k, side, r, c, :, target] = got[first : first + t].astype(bf16)
            return 0

        lax.fori_loop(0, 2 * per_half, column, 0)
        for r in range(1, rows):
            a_copy(k, r).start()
        for c in range(1, cols):
            b_copy(k, c).start()

    def combine(k):
        for r in range(1, rows):
            a_copy(k, r).wait_recv()
        for c in range(1, cols):
            total = part[k, 0, 0, c].astype(f32)
            for r in range(1, rows):
                total = total + rec_a[k, r, c].astype(f32)
            sum_a[k, c] = total.astype(bf16)
            c_copy(k, c).start()
        for c in range(1, cols):
            b_copy(k, c).wait_recv()
        for r in range(1, rows):
            total = part[k, 1, r, 0].astype(f32)
            for c in range(1, cols):
                total = total + rec_b[k, c, r].astype(f32)
            sum_b[k, r] = total.astype(bf16)
            d_copy(k, r).start()

    def activate(k):
        for c in range(1, cols):
            c_copy(k, c).wait_recv()
        for r in range(1, rows):
            d_copy(k, r).wait_recv()
        for side in range(2):
            total = acc[k, side]
            if side == 0:
                for r in range(1, rows):
                    total = total + rec_a[k, r, 0].astype(f32)
                for c in range(1, cols):
                    total = total + fin_a[k, c].astype(f32)
            else:
                for c in range(1, cols):
                    total = total + rec_b[k, c, 0].astype(f32)
                for r in range(1, rows):
                    total = total + fin_b[k, r].astype(f32)
            gate = total[:, :half]
            hbuf[k, at_slot(0, 0), pl.ds(side * half, half)] = (
                gate / (1.0 + jnp.exp(-gate)) * total[:, half:]
            ).astype(bf16)
        for r, c in edges:
            h_copy(k, r, c).start()

    def relay(k):
        for r, c in edges:
            h_copy(k, r, c).wait_recv()
        for r, c in corners:
            relay_a(k, r, c).start()
            relay_b(k, r, c).start()

    down_tile = tile_of(out_cols, 512)

    def emit(k):
        for r, c in corners:
            relay_a(k, r, c).wait_recv()
            relay_b(k, r, c).wait_recv()

        def column(j, _):
            where = pl.ds(pl.multiple_of(j * down_tile, down_tile), down_tile)
            osend[k, :, where] = jnp.dot(hbuf[k], wd[:, where], preferred_element_type=f32).astype(bf16)
            return 0

        lax.fori_loop(0, out_cols // down_tile, column, 0)
        for r, c in others:
            o_copy(k, r, c, (row, col)).start()
        o_own(k).start()

    stages = (project, combine, activate, relay, emit)

    def step(s, _):
        for lag, stage in enumerate(stages):
            k = s - lag

            @pl.when(jnp.logical_and(k >= 0, k < chunks))
            def _():
                stage(k)

            if lag == 0:

                @pl.when(s + AHEAD < chunks)
                def _():
                    send_tokens(s + AHEAD)

                @pl.when(s == 0)
                def _():
                    loads[2].wait()

        return 0

    lax.fori_loop(0, chunks + len(stages) - 1, step, 0)

    def finish(k, _):
        o_own(k).wait()
        for r, c in others:
            x_copy(k, r, c).wait_send()
            o_copy(k, r, c, (row, col)).wait_send()
            o_copy(k, r, c, up(r, c)).wait_recv()
        for r in range(1, rows):
            a_copy(k, r).wait_send()
            d_copy(k, r).wait_send()
        for c in range(1, cols):
            b_copy(k, c).wait_send()
            c_copy(k, c).wait_send()
        for r, c in edges:
            h_copy(k, r, c).wait_send()
        for r, c in corners:
            relay_a(k, r, c).wait_send()
            relay_b(k, r, c).wait_send()
        return 0

    lax.fori_loop(0, chunks, finish, 0)


def solution(mesh):
    rows, cols = mesh.shape["row"], mesh.shape["col"]
    n = rows * cols

    def shards(tokens, w_gate, w_up, w_down):
        count, width = tokens.shape
        features, hidden = w_gate.shape
        out_cols = w_down.shape[1]
        chunks = CHUNKS
        t = count // chunks
        bf16 = jnp.bfloat16
        any_space = pl.BlockSpec(memory_space=pl.ANY)

        def sems(*shape):
            return pltpu.SemaphoreType.DMA((2, chunks, *shape))

        return pl.pallas_call(
            functools.partial(kernel, rows, cols, chunks),
            out_shape=jax.ShapeDtypeStruct((count, width), bf16),
            in_specs=[any_space] * 4,
            out_specs=any_space,
            scratch_shapes=[
                pltpu.VMEM((features, hidden), bf16),
                pltpu.VMEM((features, hidden), bf16),
                pltpu.VMEM((hidden, out_cols), bf16),
                pltpu.VMEM((chunks, n * t, features), bf16),
                pltpu.VMEM((chunks, 2, t, hidden), jnp.float32),
                pltpu.VMEM((chunks, 2, rows, cols, t, hidden), bf16),
                pltpu.VMEM((chunks, rows, cols, t, hidden), bf16),
                pltpu.VMEM((chunks, cols, rows, t, hidden), bf16),
                pltpu.VMEM((chunks, cols, t, hidden), bf16),
                pltpu.VMEM((chunks, rows, t, hidden), bf16),
                pltpu.VMEM((chunks, cols, t, hidden), bf16),
                pltpu.VMEM((chunks, rows, t, hidden), bf16),
                pltpu.VMEM((chunks, n * t, hidden), bf16),
                pltpu.VMEM((chunks, n * t, out_cols), bf16),
                pltpu.SemaphoreType.DMA((3,)),
                sems(n), sems(rows), sems(cols), sems(cols), sems(rows),
                sems(n), sems(n), sems(n), sems(n),
            ],
            compiler_params=pltpu.CompilerParams(collective_id=0, has_side_effects=True),
        )(tokens, w_gate, w_up, w_down)

    in_specs = (
        P(("dp", "row", "col"), None),
        P(("row", "col"), None),
        P(("row", "col"), None),
        P(None, ("row", "col")),
    )
    out_specs = P(("dp", "row", "col"), None)
    return jax.shard_map(shards, mesh=mesh, in_specs=in_specs, out_specs=out_specs, check_vma=False)
```

```python
import functools

import jax
import jax.numpy as jnp
from jax import lax
from jax.experimental import pallas as pl
from jax.experimental.pallas import tpu as pltpu
from jax.sharding import PartitionSpec as P

MESH = pl.DeviceIdType.MESH
CHUNKS = 4
AHEAD = 2
EARLY_HOPS = 2


def tile_of(width, most):
    tile = min(width, most)
    while width % tile:
        tile //= 2
    return tile


def kernel(
    groups, rows, cols, chunks,
    x_ref, wg_ref, wu_ref, wd_ref, out_ref,
    wg, wu, wa, wb, xbuf, acc, part, rec_a, rec_b, sum_a, sum_b, fin_a, fin_b, ha, hb, oa, ob,
    w_sem, fa_sem, fb_sem, up_sem, down_sem, land_sem, mate_sem,
    x_sem, a_sem, b_sem, c_sem, d_sem, ha_sem, hb_sem, oa_sem, ob_sem,
):
    n = rows * cols
    row, col = lax.axis_index("row"), lax.axis_index("col")
    group = lax.axis_index("dp")
    mates = 2 - groups % 2
    planes = groups // mates
    plane, core = group // mates, lax.rem(group, mates)
    t = x_ref.shape[0] // chunks
    features, hidden = wg.shape
    half = hidden // 2
    side_cols = wa.shape[2]
    share = hidden // groups
    bf16, f32 = jnp.bfloat16, jnp.float32

    def up(r, c):
        return lax.rem(row + r, rows), lax.rem(col + c, cols)

    def down(r, c):
        return lax.rem(row + rows - r, rows), lax.rem(col + cols - c, cols)

    def shard(rc, width):
        return pl.ds(pl.multiple_of((rc[0] * cols + rc[1]) * width, width), width)

    def remote(src, dst, sems, index, to):
        return pltpu.make_async_remote_copy(
            src_ref=src, dst_ref=dst,
            send_sem=sems.at[(0, *index)], recv_sem=sems.at[(1, *index)],
            device_id={"row": to[0], "col": to[1]}, device_id_type=MESH,
        )

    def tok(k):
        return pl.ds(pl.multiple_of(k * t, t), t)

    slots = [(r, c) for r in range(rows) for c in range(cols)]
    others = slots[1:]

    def at_slot(r, c):
        return pl.ds((r * cols + c) * t, t)

    def x_copy(k, r, c):
        to = up(r, c)
        return remote(
            x_ref.at[tok(k), shard(to, features)], xbuf.at[k, at_slot(r, c)],
            x_sem, (k, r * cols + c), to,
        )

    def x_own(k):
        return pltpu.make_async_copy(
            x_ref.at[tok(k), shard((row, col), features)], xbuf.at[k, at_slot(0, 0)], x_sem.at[1, k, 0]
        )

    def a_copy(k, r):
        return remote(part.at[k, 0, r], rec_a.at[k, r], a_sem, (k, r), down(r, 0))

    def b_copy(k, c):
        return remote(part.at[k, 1, :, c], rec_b.at[k, c], b_sem, (k, c), down(0, c))

    def c_copy(k, c):
        return remote(sum_a.at[k, c], fin_a.at[k, c], c_sem, (k, c), down(0, c))

    def d_copy(k, r):
        return remote(sum_b.at[k, r], fin_b.at[k, r], d_sem, (k, r), down(r, 0))

    def share_of(g):
        return pl.ds(pl.multiple_of(g * share, share), share)

    def fetch_a(c):
        return remote(
            wd_ref.at[share_of(group), pl.ds(0, side_cols)], wa.at[c, share_of(group)],
            fa_sem, (c,), down(0, c),
        )

    def fetch_b(r):
        return remote(
            wd_ref.at[share_of(group), pl.ds(side_cols, side_cols)], wb.at[r, share_of(group)],
            fb_sem, (r,), down(r, 0),
        )

    blocks = [(wa, c, c) for c in range(1, cols)] + [(wb, r, cols + r) for r in range(1, rows)]

    def pass_on(source, block, sems, to_plane):
        ref, slot, index = block
        region = ref.at[slot, share_of(source * mates + core)]
        return pltpu.make_async_remote_copy(
            src_ref=region, dst_ref=region,
            send_sem=sems.at[source, index], recv_sem=land_sem.at[source, index],
            device_id={"dp": to_plane * mates + core}, device_id_type=MESH,
        )

    def to_mate(source, block, whose):
        ref, slot, index = block
        region = ref.at[slot, share_of(source * mates + whose)]
        return pltpu.make_async_remote_copy(
            src_ref=region, dst_ref=region,
            send_sem=mate_sem.at[0, source, index], recv_sem=mate_sem.at[1, source, index],
            device_id={"dp": plane * mates + (mates - 1 - core)}, device_id_type=MESH,
        )

    def spread(source, upward, downward):
        for block in blocks:
            if mates > 1:
                to_mate(source, block, core).start()
            if upward:

                @pl.when(plane + 1 < planes)
                def _():
                    pass_on(source, block, up_sem, plane + 1).start()

            if downward:

                @pl.when(plane > 0)
                def _():
                    pass_on(source, block, down_sem, plane - 1).start()

    def hop(h):
        below, above = plane - h, plane + h

        @pl.when(below >= 0)
        def _():
            for block in blocks:
                pass_on(below, block, up_sem, plane).wait_recv()
            spread(below, True, False)

        @pl.when(above < planes)
        def _():
            for block in blocks:
                pass_on(above, block, down_sem, plane).wait_recv()
            spread(above, False, True)

    def last_hops():
        def more(h, _):
            hop(h)
            return 0

        lax.fori_loop(EARLY_HOPS + 1, planes, more, 0)
        if mates > 1:

            def landed(z, _):
                for block in blocks:
                    to_mate(z, block, mates - 1 - core).wait_recv()
                return 0

            lax.fori_loop(0, planes, landed, 0)

    def sent(z, _):
        for block in blocks:
            if mates > 1:
                to_mate(z, block, core).wait_send()

            @pl.when(jnp.logical_and(plane + 1 < planes, z <= plane))
            def _():
                pass_on(z, block, up_sem, plane).wait_send()

            @pl.when(jnp.logical_and(plane > 0, z >= plane))
            def _():
                pass_on(z, block, down_sem, plane).wait_send()

        return 0

    def ha_copy(k, r):
        return remote(ha.at[k, pl.ds(0, t)], ha.at[k, pl.ds(r * t, t)], ha_sem, (k, r), up(r, 0))

    def hb_copy(k, c):
        return remote(hb.at[k, pl.ds(0, t)], hb.at[k, pl.ds(c * t, t)], hb_sem, (k, c), up(0, c))

    def out_at(k, rc, side):
        start = (rc[0] * cols + rc[1]) * 2 * side_cols + side * side_cols
        return out_ref.at[tok(k), pl.ds(pl.multiple_of(start, side_cols), side_cols)]

    def oa_copy(k, r, c, columns_of):
        return remote(
            oa.at[k, c, pl.ds(r * t, t)], out_at(k, columns_of, 0), oa_sem, (k, r, c), down(r, 0)
        )

    def ob_copy(k, r, c, columns_of):
        return remote(
            ob.at[k, r, pl.ds(c * t, t)], out_at(k, columns_of, 1), ob_sem, (k, r, c), down(0, c)
        )

    def oa_own(k, c):
        return pltpu.make_async_copy(
            oa.at[k, c, pl.ds(0, t)], out_at(k, up(0, c), 0), oa_sem.at[1, k, 0, c]
        )

    def ob_own(k, r):
        return pltpu.make_async_copy(
            ob.at[k, r, pl.ds(0, t)], out_at(k, up(r, 0), 1), ob_sem.at[1, k, r, 0]
        )

    loads = [
        pltpu.make_async_copy(wg_ref, wg, w_sem.at[0]),
        pltpu.make_async_copy(wu_ref, wu, w_sem.at[1]),
        pltpu.make_async_copy(wd_ref.at[:, pl.ds(0, side_cols)], wa.at[0], w_sem.at[2]),
        pltpu.make_async_copy(wd_ref.at[:, pl.ds(side_cols, side_cols)], wb.at[0], w_sem.at[3]),
    ]

    barrier = pltpu.get_barrier_semaphore()
    for r, c in others:
        to = up(r, c)
        pl.semaphore_signal(barrier, inc=1, device_id={"row": to[0], "col": to[1]}, device_id_type=MESH)
    def greet(g):
        pl.semaphore_signal(barrier, inc=1, device_id={"dp": g}, device_id_type=MESH)

    pl.when(plane > 0)(lambda: greet(group - mates))
    pl.when(plane + 1 < planes)(lambda: greet(group + mates))
    if mates > 1:
        greet(plane * mates + (mates - 1 - core))
    neighbours = (plane > 0).astype(jnp.int32) + (plane + 1 < planes).astype(jnp.int32)
    pl.semaphore_wait(barrier, n - 1 + mates - 1 + neighbours)

    for c in range(1, cols):
        fetch_a(c).start()
    for r in range(1, rows):
        fetch_b(r).start()

    def send_tokens(k):
        for r, c in others:
            x_copy(k, r, c).start()

    for k in range(min(AHEAD, chunks)):
        send_tokens(k)
    for k in range(chunks):
        x_own(k).start()
    for load in loads:
        load.start()
    for c in range(1, cols):
        fetch_a(c).wait_recv()
    for r in range(1, rows):
        fetch_b(r).wait_recv()
    spread(plane, True, True)
    for load in loads:
        load.wait()

    tile = tile_of(half, 512)
    per_half = half // tile

    def project(k):
        x_own(k).wait()
        for r, c in others:
            x_copy(k, r, c).wait_recv()

        def column(j, _):
            side, at = j // per_half, lax.rem(j, per_half) * tile
            source = pl.ds(pl.multiple_of(j * tile, tile), tile)
            for w, base in ((wg, 0), (wu, half)):
                target = pl.ds(pl.multiple_of(base + at, tile), tile)
                got = jnp.dot(xbuf[k], w[:, source], preferred_element_type=f32)
                acc[k, side, :, target] = got[:t]
                for r, c in others:
                    first = (r * cols + c) * t
                    part[k, side, r, c, :, target] = got[first : first + t].astype(bf16)
            return 0

        lax.fori_loop(0, 2 * per_half, column, 0)
        for r in range(1, rows):
            a_copy(k, r).start()
        for c in range(1, cols):
            b_copy(k, c).start()

    def combine(k):
        for r in range(1, rows):
            a_copy(k, r).wait_recv()
        for c in range(1, cols):
            total = part[k, 0, 0, c].astype(f32)
            for r in range(1, rows):
                total = total + rec_a[k, r, c].astype(f32)
            sum_a[k, c] = total.astype(bf16)
            c_copy(k, c).start()
        for c in range(1, cols):
            b_copy(k, c).wait_recv()
        for r in range(1, rows):
            total = part[k, 1, r, 0].astype(f32)
            for c in range(1, cols):
                total = total + rec_b[k, c, r].astype(f32)
            sum_b[k, r] = total.astype(bf16)
            d_copy(k, r).start()

    def activate(k):
        for c in range(1, cols):
            c_copy(k, c).wait_recv()
        for r in range(1, rows):
            d_copy(k, r).wait_recv()
        for side in range(2):
            total = acc[k, side]
            if side == 0:
                for r in range(1, rows):
                    total = total + rec_a[k, r, 0].astype(f32)
                for c in range(1, cols):
                    total = total + fin_a[k, c].astype(f32)
            else:
                for c in range(1, cols):
                    total = total + rec_b[k, c, 0].astype(f32)
                for r in range(1, rows):
                    total = total + fin_b[k, r].astype(f32)
            gate = total[:, :half]
            done = (gate / (1.0 + jnp.exp(-gate)) * total[:, half:]).astype(bf16)
            ha[k, pl.ds(0, t), pl.ds(side * half, half)] = done
            hb[k, pl.ds(0, t), pl.ds(side * half, half)] = done
        for r in range(1, rows):
            ha_copy(k, r).start()
        for c in range(1, cols):
            hb_copy(k, c).start()

    out_tile = tile_of(side_cols, 512)
    out_tiles = side_cols // out_tile

    def emit(k):
        for r in range(1, rows):
            ha_copy(k, r).wait_recv()

        def columns_a(j, _):
            c = j // out_tiles
            where = pl.ds(pl.multiple_of(lax.rem(j, out_tiles) * out_tile, out_tile), out_tile)
            oa[k, c, :, where] = jnp.dot(
                ha[k], wa[c, :, where], preferred_element_type=f32
            ).astype(bf16)
            return 0

        lax.fori_loop(0, cols * out_tiles, columns_a, 0)
        for c in range(cols):
            for r in range(1, rows):
                oa_copy(k, r, c, up(0, c)).start()
        for c in range(1, cols):
            hb_copy(k, c).wait_recv()

        def columns_b(j, _):
            r = j // out_tiles
            where = pl.ds(pl.multiple_of(lax.rem(j, out_tiles) * out_tile, out_tile), out_tile)
            ob[k, r, :, where] = jnp.dot(
                hb[k], wb[r, :, where], preferred_element_type=f32
            ).astype(bf16)
            return 0

        lax.fori_loop(0, rows * out_tiles, columns_b, 0)
        for r in range(rows):
            for c in range(1, cols):
                ob_copy(k, r, c, up(r, 0)).start()
        for c in range(cols):
            oa_own(k, c).start()
        for r in range(rows):
            ob_own(k, r).start()

    stages = (project, combine, activate, emit)

    def step(s, _):
        for lag, stage in enumerate(stages):
            k = s - lag

            @pl.when(jnp.logical_and(k >= 0, k < chunks))
            def _():
                stage(k)

            if lag == 0:

                @pl.when(s + AHEAD < chunks)
                def _():
                    send_tokens(s + AHEAD)

                for h in range(1, min(EARLY_HOPS, planes - 1) + 1):
                    pl.when(s == h)(lambda h=h: hop(h))

                pl.when(s == len(stages) - 1)(last_hops)

        return 0

    lax.fori_loop(0, chunks + len(stages) - 1, step, 0)

    def finish(k, _):
        for r, c in others:
            x_copy(k, r, c).wait_send()
        for r, c in slots:
            if r:
                oa_copy(k, r, c, up(0, c)).wait_send()
                oa_copy(k, r, c, up(r, c)).wait_recv()
            else:
                oa_own(k, c).wait()
            if c:
                ob_copy(k, r, c, up(r, 0)).wait_send()
                ob_copy(k, r, c, up(r, c)).wait_recv()
            else:
                ob_own(k, r).wait()
        for r in range(1, rows):
            a_copy(k, r).wait_send()
            d_copy(k, r).wait_send()
            ha_copy(k, r).wait_send()
        for c in range(1, cols):
            b_copy(k, c).wait_send()
            c_copy(k, c).wait_send()
            hb_copy(k, c).wait_send()
        return 0

    lax.fori_loop(0, chunks, finish, 0)
    for c in range(1, cols):
        fetch_a(c).wait_send()
    for r in range(1, rows):
        fetch_b(r).wait_send()
    lax.fori_loop(0, planes, sent, 0)


def solution(mesh):
    groups, rows, cols = mesh.shape["dp"], mesh.shape["row"], mesh.shape["col"]
    planes = groups // (2 - groups % 2)
    n = rows * cols

    def shards(tokens, w_gate, w_up, w_down):
        count, width = tokens.shape
        features, hidden = w_gate.shape
        side_cols = w_down.shape[1] // 2
        chunks = CHUNKS
        t = count // chunks
        bf16 = jnp.bfloat16
        any_space = pl.BlockSpec(memory_space=pl.ANY)

        def sems(*shape):
            return pltpu.SemaphoreType.DMA((2, chunks, *shape))

        return pl.pallas_call(
            functools.partial(kernel, groups, rows, cols, chunks),
            out_shape=jax.ShapeDtypeStruct((count, width), bf16),
            in_specs=[any_space] * 4,
            out_specs=any_space,
            scratch_shapes=[
                pltpu.VMEM((features, hidden), bf16),
                pltpu.VMEM((features, hidden), bf16),
                pltpu.VMEM((cols, hidden, side_cols), bf16),
                pltpu.VMEM((rows, hidden, side_cols), bf16),
                pltpu.VMEM((chunks, n * t, features), bf16),
                pltpu.VMEM((chunks, 2, t, hidden), jnp.float32),
                pltpu.VMEM((chunks, 2, rows, cols, t, hidden), bf16),
                pltpu.VMEM((chunks, rows, cols, t, hidden), bf16),
                pltpu.VMEM((chunks, cols, rows, t, hidden), bf16),
                pltpu.VMEM((chunks, cols, t, hidden), bf16),
                pltpu.VMEM((chunks, rows, t, hidden), bf16),
                pltpu.VMEM((chunks, cols, t, hidden), bf16),
                pltpu.VMEM((chunks, rows, t, hidden), bf16),
                pltpu.VMEM((chunks, rows * t, hidden), bf16),
                pltpu.VMEM((chunks, cols * t, hidden), bf16),
                pltpu.VMEM((chunks, cols, rows * t, side_cols), bf16),
                pltpu.VMEM((chunks, rows, cols * t, side_cols), bf16),
                pltpu.SemaphoreType.DMA((4,)),
                pltpu.SemaphoreType.DMA((2, cols)),
                pltpu.SemaphoreType.DMA((2, rows)),
                pltpu.SemaphoreType.DMA((planes, cols + rows)),
                pltpu.SemaphoreType.DMA((planes, cols + rows)),
                pltpu.SemaphoreType.DMA((planes, cols + rows)),
                pltpu.SemaphoreType.DMA((2, planes, cols + rows)),
                sems(n), sems(rows), sems(cols), sems(cols), sems(rows),
                sems(rows), sems(cols), sems(rows, cols), sems(rows, cols),
            ],
            compiler_params=pltpu.CompilerParams(collective_id=0, has_side_effects=True),
        )(tokens, w_gate, w_up, w_down)

    in_specs = (
        P(("dp", "row", "col"), None),
        P(("row", "col"), None),
        P(("row", "col"), None),
        P(None, ("row", "col")),
    )
    out_specs = P(("dp", "row", "col"), None)
    return jax.shard_map(shards, mesh=mesh, in_specs=in_specs, out_specs=out_specs, check_vma=False)
```

```python
import functools

import jax
import jax.numpy as jnp
from jax import lax
from jax.experimental import pallas as pl
from jax.experimental.pallas import tpu as pltpu
from jax.sharding import PartitionSpec as P

MESH = pl.DeviceIdType.MESH
CHUNKS = 4
AHEAD = 3
EARLY_HOPS = 2


def tile_of(width, most):
    tile = min(width, most)
    while width % tile:
        tile //= 2
    return tile


def kernel(
    groups, rows, cols, chunks,
    x_ref, wg_ref, wu_ref, wd_ref, out_ref,
    wg, wu, wa, wb, xbuf, acc, part, rec_a, rec_b, sum_a, sum_b, fin_a, fin_b, ha, hb, oa, ob,
    w_sem, fa_sem, fb_sem, up_sem, down_sem, land_sem, mate_sem,
    x_sem, a_sem, b_sem, c_sem, d_sem, ha_sem, hb_sem, oa_sem, ob_sem,
):
    n = rows * cols
    row, col = lax.axis_index("row"), lax.axis_index("col")
    group = lax.axis_index("dp")
    mates = 2 - groups % 2
    planes = groups // mates
    plane, core = group // mates, lax.rem(group, mates)
    t = x_ref.shape[0] // chunks
    features, hidden = wg.shape
    half = hidden // 2
    side_cols = wa.shape[2]
    share = hidden // groups
    bf16, f32 = jnp.bfloat16, jnp.float32

    def up(r, c):
        return lax.rem(row + r, rows), lax.rem(col + c, cols)

    def down(r, c):
        return lax.rem(row + rows - r, rows), lax.rem(col + cols - c, cols)

    def shard(rc, width):
        return pl.ds(pl.multiple_of((rc[0] * cols + rc[1]) * width, width), width)

    def remote(src, dst, sems, index, to):
        return pltpu.make_async_remote_copy(
            src_ref=src, dst_ref=dst,
            send_sem=sems.at[(0, *index)], recv_sem=sems.at[(1, *index)],
            device_id={"row": to[0], "col": to[1]}, device_id_type=MESH,
        )

    def tok(k):
        return pl.ds(pl.multiple_of(k * t, t), t)

    slots = [(r, c) for r in range(rows) for c in range(cols)]
    others = slots[1:]
    by_reach = others[::-1]

    def at_slot(r, c):
        return pl.ds((r * cols + c) * t, t)

    def x_copy(k, r, c):
        to = up(r, c)
        return remote(
            x_ref.at[tok(k), shard(to, features)], xbuf.at[k, at_slot(r, c)],
            x_sem, (k, r * cols + c), to,
        )

    def x_own(k):
        return pltpu.make_async_copy(
            x_ref.at[tok(k), shard((row, col), features)], xbuf.at[k, at_slot(0, 0)], x_sem.at[1, k, 0]
        )

    def a_copy(k, r):
        return remote(part.at[k, 0, r], rec_a.at[k, r], a_sem, (k, r), down(r, 0))

    def b_copy(k, c):
        return remote(part.at[k, 1, :, c], rec_b.at[k, c], b_sem, (k, c), down(0, c))

    def c_copy(k, c):
        return remote(sum_a.at[k, c], fin_a.at[k, c], c_sem, (k, c), down(0, c))

    def d_copy(k, r):
        return remote(sum_b.at[k, r], fin_b.at[k, r], d_sem, (k, r), down(r, 0))

    def share_of(g):
        return pl.ds(pl.multiple_of(g * share, share), share)

    def fetch_a(c):
        return remote(
            wd_ref.at[share_of(group), pl.ds(0, side_cols)], wa.at[c, share_of(group)],
            fa_sem, (c,), down(0, c),
        )

    def fetch_b(r):
        return remote(
            wd_ref.at[share_of(group), pl.ds(side_cols, side_cols)], wb.at[r, share_of(group)],
            fb_sem, (r,), down(r, 0),
        )

    blocks = [(wa, c, c) for c in range(1, cols)] + [(wb, r, cols + r) for r in range(1, rows)]

    def pass_on(source, block, sems, to_plane):
        ref, slot, index = block
        region = ref.at[slot, share_of(source * mates + core)]
        return pltpu.make_async_remote_copy(
            src_ref=region, dst_ref=region,
            send_sem=sems.at[source, index], recv_sem=land_sem.at[source, index],
            device_id={"dp": to_plane * mates + core}, device_id_type=MESH,
        )

    def to_mate(source, block, whose):
        ref, slot, index = block
        region = ref.at[slot, share_of(source * mates + whose)]
        return pltpu.make_async_remote_copy(
            src_ref=region, dst_ref=region,
            send_sem=mate_sem.at[0, source, index], recv_sem=mate_sem.at[1, source, index],
            device_id={"dp": plane * mates + (mates - 1 - core)}, device_id_type=MESH,
        )

    def spread(source, upward, downward):
        for block in blocks:
            if mates > 1:
                to_mate(source, block, core).start()
            if upward:

                @pl.when(plane + 1 < planes)
                def _():
                    pass_on(source, block, up_sem, plane + 1).start()

            if downward:

                @pl.when(plane > 0)
                def _():
                    pass_on(source, block, down_sem, plane - 1).start()

    def hop(h):
        below, above = plane - h, plane + h

        @pl.when(below >= 0)
        def _():
            for block in blocks:
                pass_on(below, block, up_sem, plane).wait_recv()
            spread(below, True, False)

        @pl.when(above < planes)
        def _():
            for block in blocks:
                pass_on(above, block, down_sem, plane).wait_recv()
            spread(above, False, True)

    def last_hops():
        def more(h, _):
            hop(h)
            return 0

        lax.fori_loop(EARLY_HOPS + 1, planes, more, 0)
        if mates > 1:

            def landed(z, _):
                for block in blocks:
                    to_mate(z, block, mates - 1 - core).wait_recv()
                return 0

            lax.fori_loop(0, planes, landed, 0)

    def sent(z, _):
        for block in blocks:
            if mates > 1:
                to_mate(z, block, core).wait_send()

            @pl.when(jnp.logical_and(plane + 1 < planes, z <= plane))
            def _():
                pass_on(z, block, up_sem, plane).wait_send()

            @pl.when(jnp.logical_and(plane > 0, z >= plane))
            def _():
                pass_on(z, block, down_sem, plane).wait_send()

        return 0

    def ha_copy(k, r):
        return remote(ha.at[k, pl.ds(0, t)], ha.at[k, pl.ds(r * t, t)], ha_sem, (k, r), up(r, 0))

    def hb_copy(k, c):
        return remote(hb.at[k, pl.ds(0, t)], hb.at[k, pl.ds(c * t, t)], hb_sem, (k, c), up(0, c))

    def out_at(k, rc, side):
        start = (rc[0] * cols + rc[1]) * 2 * side_cols + side * side_cols
        return out_ref.at[tok(k), pl.ds(pl.multiple_of(start, side_cols), side_cols)]

    def oa_copy(k, r, c, columns_of):
        return remote(
            oa.at[k, c, pl.ds(r * t, t)], out_at(k, columns_of, 0), oa_sem, (k, r, c), down(r, 0)
        )

    def ob_copy(k, r, c, columns_of):
        return remote(
            ob.at[k, r, pl.ds(c * t, t)], out_at(k, columns_of, 1), ob_sem, (k, r, c), down(0, c)
        )

    def oa_own(k, c):
        return pltpu.make_async_copy(
            oa.at[k, c, pl.ds(0, t)], out_at(k, up(0, c), 0), oa_sem.at[1, k, 0, c]
        )

    def ob_own(k, r):
        return pltpu.make_async_copy(
            ob.at[k, r, pl.ds(0, t)], out_at(k, up(r, 0), 1), ob_sem.at[1, k, r, 0]
        )

    loads = [
        pltpu.make_async_copy(wg_ref, wg, w_sem.at[0]),
        pltpu.make_async_copy(wu_ref, wu, w_sem.at[1]),
        pltpu.make_async_copy(wd_ref.at[:, pl.ds(0, side_cols)], wa.at[0], w_sem.at[2]),
        pltpu.make_async_copy(wd_ref.at[:, pl.ds(side_cols, side_cols)], wb.at[0], w_sem.at[3]),
    ]

    barrier = pltpu.get_barrier_semaphore()
    for r, c in others:
        to = up(r, c)
        pl.semaphore_signal(barrier, inc=1, device_id={"row": to[0], "col": to[1]}, device_id_type=MESH)
    def greet(g):
        pl.semaphore_signal(barrier, inc=1, device_id={"dp": g}, device_id_type=MESH)

    pl.when(plane > 0)(lambda: greet(group - mates))
    pl.when(plane + 1 < planes)(lambda: greet(group + mates))
    if mates > 1:
        greet(plane * mates + (mates - 1 - core))
    neighbours = (plane > 0).astype(jnp.int32) + (plane + 1 < planes).astype(jnp.int32)
    pl.semaphore_wait(barrier, n - 1 + mates - 1 + neighbours)

    for c in range(1, cols):
        fetch_a(c).start()
    for r in range(1, rows):
        fetch_b(r).start()

    def send_tokens(k):
        for r, c in by_reach:
            x_copy(k, r, c).start()

    for k in range(min(AHEAD, chunks)):
        send_tokens(k)
    for k in range(chunks):
        x_own(k).start()
    for load in loads:
        load.start()
    for c in range(1, cols):
        fetch_a(c).wait_recv()
    for r in range(1, rows):
        fetch_b(r).wait_recv()
    spread(plane, True, True)
    for load in loads:
        load.wait()

    tile = tile_of(half, 512)
    per_half = half // tile

    def project(k):
        x_own(k).wait()
        for r, c in others:
            x_copy(k, r, c).wait_recv()

        def column(j, _):
            side, at = j // per_half, lax.rem(j, per_half) * tile
            source = pl.ds(pl.multiple_of(j * tile, tile), tile)
            for w, base in ((wg, 0), (wu, half)):
                target = pl.ds(pl.multiple_of(base + at, tile), tile)
                got = jnp.dot(xbuf[k], w[:, source], preferred_element_type=f32)
                acc[k, side, :, target] = got[:t]
                for r, c in others:
                    first = (r * cols + c) * t
                    part[k, side, r, c, :, target] = got[first : first + t].astype(bf16)
            return 0

        lax.fori_loop(0, 2 * per_half, column, 0)
        for r in range(1, rows):
            a_copy(k, r).start()
        for c in range(1, cols):
            b_copy(k, c).start()

    def combine(k):
        for r in range(1, rows):
            a_copy(k, r).wait_recv()
        for c in range(1, cols):
            total = part[k, 0, 0, c].astype(f32)
            for r in range(1, rows):
                total = total + rec_a[k, r, c].astype(f32)
            sum_a[k, c] = total.astype(bf16)
            c_copy(k, c).start()
        for c in range(1, cols):
            b_copy(k, c).wait_recv()
        for r in range(1, rows):
            total = part[k, 1, r, 0].astype(f32)
            for c in range(1, cols):
                total = total + rec_b[k, c, r].astype(f32)
            sum_b[k, r] = total.astype(bf16)
            d_copy(k, r).start()

    def activate(k):
        for c in range(1, cols):
            c_copy(k, c).wait_recv()
        for r in range(1, rows):
            d_copy(k, r).wait_recv()
        for side in range(2):
            total = acc[k, side]
            if side == 0:
                for r in range(1, rows):
                    total = total + rec_a[k, r, 0].astype(f32)
                for c in range(1, cols):
                    total = total + fin_a[k, c].astype(f32)
            else:
                for c in range(1, cols):
                    total = total + rec_b[k, c, 0].astype(f32)
                for r in range(1, rows):
                    total = total + fin_b[k, r].astype(f32)
            gate = total[:, :half]
            done = (gate / (1.0 + jnp.exp(-gate)) * total[:, half:]).astype(bf16)
            ha[k, pl.ds(0, t), pl.ds(side * half, half)] = done
            hb[k, pl.ds(0, t), pl.ds(side * half, half)] = done
        for r in range(1, rows):
            ha_copy(k, r).start()
        for c in range(1, cols):
            hb_copy(k, c).start()

    out_tile = tile_of(side_cols, 512)
    out_tiles = side_cols // out_tile

    def emit(k):
        for r in range(1, rows):
            ha_copy(k, r).wait_recv()

        def columns_a(j, _):
            c = j // out_tiles
            where = pl.ds(pl.multiple_of(lax.rem(j, out_tiles) * out_tile, out_tile), out_tile)
            oa[k, c, :, where] = jnp.dot(
                ha[k], wa[c, :, where], preferred_element_type=f32
            ).astype(bf16)
            return 0

        lax.fori_loop(0, cols * out_tiles, columns_a, 0)
        for c in range(cols):
            for r in range(1, rows):
                oa_copy(k, r, c, up(0, c)).start()
        for c in range(1, cols):
            hb_copy(k, c).wait_recv()

        def columns_b(j, _):
            r = j // out_tiles
            where = pl.ds(pl.multiple_of(lax.rem(j, out_tiles) * out_tile, out_tile), out_tile)
            ob[k, r, :, where] = jnp.dot(
                hb[k], wb[r, :, where], preferred_element_type=f32
            ).astype(bf16)
            return 0

        lax.fori_loop(0, rows * out_tiles, columns_b, 0)
        for r in range(rows):
            for c in range(1, cols):
                ob_copy(k, r, c, up(r, 0)).start()
        for c in range(cols):
            oa_own(k, c).start()
        for r in range(rows):
            ob_own(k, r).start()

    stages = (project, combine, activate, emit)

    def step(s, _):
        for lag, stage in enumerate(stages):
            k = s - lag

            @pl.when(jnp.logical_and(k >= 0, k < chunks))
            def _():
                stage(k)

            if lag == 0:

                @pl.when(s + AHEAD < chunks)
                def _():
                    send_tokens(s + AHEAD)

                for h in range(1, min(EARLY_HOPS, planes - 1) + 1):
                    pl.when(s == h)(lambda h=h: hop(h))

                pl.when(s == len(stages) - 1)(last_hops)

        return 0

    lax.fori_loop(0, chunks + len(stages) - 1, step, 0)

    def finish(k, _):
        for r, c in others:
            x_copy(k, r, c).wait_send()
        for r, c in slots:
            if r:
                oa_copy(k, r, c, up(0, c)).wait_send()
                oa_copy(k, r, c, up(r, c)).wait_recv()
            else:
                oa_own(k, c).wait()
            if c:
                ob_copy(k, r, c, up(r, 0)).wait_send()
                ob_copy(k, r, c, up(r, c)).wait_recv()
            else:
                ob_own(k, r).wait()
        for r in range(1, rows):
            a_copy(k, r).wait_send()
            d_copy(k, r).wait_send()
            ha_copy(k, r).wait_send()
        for c in range(1, cols):
            b_copy(k, c).wait_send()
            c_copy(k, c).wait_send()
            hb_copy(k, c).wait_send()
        return 0

    lax.fori_loop(0, chunks, finish, 0)
    for c in range(1, cols):
        fetch_a(c).wait_send()
    for r in range(1, rows):
        fetch_b(r).wait_send()
    lax.fori_loop(0, planes, sent, 0)


def solution(mesh):
    groups, rows, cols = mesh.shape["dp"], mesh.shape["row"], mesh.shape["col"]
    planes = groups // (2 - groups % 2)
    n = rows * cols

    def shards(tokens, w_gate, w_up, w_down):
        count, width = tokens.shape
        features, hidden = w_gate.shape
        side_cols = w_down.shape[1] // 2
        chunks = CHUNKS
        t = count // chunks
        bf16 = jnp.bfloat16
        any_space = pl.BlockSpec(memory_space=pl.ANY)

        def sems(*shape):
            return pltpu.SemaphoreType.DMA((2, chunks, *shape))

        return pl.pallas_call(
            functools.partial(kernel, groups, rows, cols, chunks),
            out_shape=jax.ShapeDtypeStruct((count, width), bf16),
            in_specs=[any_space] * 4,
            out_specs=any_space,
            scratch_shapes=[
                pltpu.VMEM((features, hidden), bf16),
                pltpu.VMEM((features, hidden), bf16),
                pltpu.VMEM((cols, hidden, side_cols), bf16),
                pltpu.VMEM((rows, hidden, side_cols), bf16),
                pltpu.VMEM((chunks, n * t, features), bf16),
                pltpu.VMEM((chunks, 2, t, hidden), jnp.float32),
                pltpu.VMEM((chunks, 2, rows, cols, t, hidden), bf16),
                pltpu.VMEM((chunks, rows, cols, t, hidden), bf16),
                pltpu.VMEM((chunks, cols, rows, t, hidden), bf16),
                pltpu.VMEM((chunks, cols, t, hidden), bf16),
                pltpu.VMEM((chunks, rows, t, hidden), bf16),
                pltpu.VMEM((chunks, cols, t, hidden), bf16),
                pltpu.VMEM((chunks, rows, t, hidden), bf16),
                pltpu.VMEM((chunks, rows * t, hidden), bf16),
                pltpu.VMEM((chunks, cols * t, hidden), bf16),
                pltpu.VMEM((chunks, cols, rows * t, side_cols), bf16),
                pltpu.VMEM((chunks, rows, cols * t, side_cols), bf16),
                pltpu.SemaphoreType.DMA((4,)),
                pltpu.SemaphoreType.DMA((2, cols)),
                pltpu.SemaphoreType.DMA((2, rows)),
                pltpu.SemaphoreType.DMA((planes, cols + rows)),
                pltpu.SemaphoreType.DMA((planes, cols + rows)),
                pltpu.SemaphoreType.DMA((planes, cols + rows)),
                pltpu.SemaphoreType.DMA((2, planes, cols + rows)),
                sems(n), sems(rows), sems(cols), sems(cols), sems(rows),
                sems(rows), sems(cols), sems(rows, cols), sems(rows, cols),
            ],
            compiler_params=pltpu.CompilerParams(collective_id=0, has_side_effects=True),
        )(tokens, w_gate, w_up, w_down)

    in_specs = (
        P(("dp", "row", "col"), None),
        P(("row", "col"), None),
        P(("row", "col"), None),
        P(None, ("row", "col")),
    )
    out_specs = P(("dp", "row", "col"), None)
    return jax.shard_map(shards, mesh=mesh, in_specs=in_specs, out_specs=out_specs, check_vma=False)
```
